256 devices in a mesh: rep: 2 (over z), tp: 16 (over y, core), sub: 8 (over x).
Axes of the slice: x: 8, y: 8, z: 2, core: 2. Of those that a mesh axis runs over, the one named last changes fastest.
The devices are a block of a 8x8x16 slice.
Arguments:
- acts: bfloat16 [2048, 16384], P(('rep', 'tp'), 'sub'), parts along dimension 0, may hold values from -6 to 6
- q_src: bfloat16 [32768, 16384], P(('rep', 'sub'), 'tp'), parts along dimension 0, may hold values from -0.046875 to 0.046875
- kv_src: bfloat16 [32768, 2048], P(('rep', 'sub'), 'tp'), parts along dimension 0, may hold values from -0.046875 to 0.046875
- q_src_heads: int32 [128], replicated, may hold values from 0 to 127, as said below
- q_tgt_heads: int32 [128], replicated, may hold values from 0 to 127, as said below
- kv_tgt_heads: int32 [16], replicated, may hold values from 0 to 7, as said below
Outputs:
- q_new: bfloat16 [32768, 16384], P(('rep', 'sub'), 'tp'), parts along dimension 0
- kv_new: bfloat16 [32768, 4096], P(('rep', 'sub'), 'tp'), parts along dimension 0
- qkv: bfloat16 [2048, 20480], P(('rep', 'sub'), 'tp'), parts along dimension 0
The draws below stay inside these ranges and needn't reach their ends.
There are 2 independent parts, one for each index of `rep`. The reference program is written for one: setup_inputs(seed, part) draws one part's arguments, and reference() takes and returns one part's arrays. A program takes and returns all parts, laid end to end along the dimension named above; an argument that names none is the same for every part. Nothing has to cross between parts.
Inputs may be any that keep to these rules, and one draw needn't show every extreme that they name: q_src_heads and q_tgt_heads are permutations. Source block t is entries t * 8 to (t + 1) * 8 - 1 of q_src_heads, target block j the same entries of q_tgt_heads. With s = 4, source block t shares exactly 2 heads with target block (t + min(1, s - 1)) mod 16 and with each target block (t + k * s) mod 16 for k from 1 to 3, and none with any other. `q_tgt_heads`: see q_src_heads. `kv_tgt_heads`: every key-value head appears exactly twice.
All inputs are finite; a program needn't handle non-finite values.
Results may differ from the reference program's by a relative error of at most 0.001.
Values may be sent and summed in bfloat16 or wider, within the bound.
A program may use at most 128 MiB of HBM per device.

```python
import jax
import jax.numpy as jnp

D = 16384
QH = 128
KVH = 8
HD = 128
TOK = 1024
QDEV = 8
KVT = 1
CDEV = 1280
CAP = 2
NSEL = 4
N_TP = 16


def query_tables(key):
    key = jax.random.fold_in(key, 11)
    key_heads = jax.random.fold_in(key, 0)
    key_group = jax.random.fold_in(key, 2)
    key_order = jax.random.fold_in(key, 3)
    head_order = jax.random.permutation(key_heads, QH).astype(jnp.int32)
    stride = N_TP // NSEL
    steps = jnp.arange(NSEL, dtype=jnp.int32)
    chosen = jnp.where(steps == 0, min(1, stride - 1), steps * stride).astype(jnp.int32)
    grouping = jax.random.permutation(key_group, QDEV).astype(jnp.int32)
    inverse = jnp.argsort(grouping).astype(jnp.int32)
    target_ids = jnp.arange(N_TP, dtype=jnp.int32)[:, None]
    position = jnp.arange(QDEV, dtype=jnp.int32)[None, :]
    source_dev = (target_ids - chosen[position // CAP]) % N_TP
    global_slot = source_dev * QDEV + inverse[position]
    order_keys = jax.random.split(key_order, N_TP)
    shuffle = jax.vmap(lambda k: jax.random.permutation(k, QDEV))(order_keys).astype(jnp.int32)
    global_slot = jnp.take_along_axis(global_slot, shuffle, axis=1)
    target_heads = head_order[global_slot.reshape(QH)]
    return (head_order, target_heads.astype(jnp.int32))


def draw_q_src_heads(key, part):
    return query_tables(key)[0]


def draw_q_tgt_heads(key, part):
    return query_tables(key)[1]


def draw_kv_tgt_heads(key, part):
    order = jax.random.permutation(jax.random.fold_in(key, 23), KVH).astype(jnp.int32)
    fixed_heads = (jnp.arange(KVH, dtype=jnp.int32) + KVH // 2) % KVH
    paired = jnp.stack([fixed_heads, order], axis=1)
    return paired.reshape(2 * KVH).astype(jnp.int32)


def shard_levels(own_key, shape, cuts, smallest, high):
    level, own = 1.0, jax.random.fold_in(own_key, 6)
    for axis_at, parts in cuts:
        heights = jnp.exp(jax.random.uniform(jax.random.fold_in(own, axis_at), (parts,), jnp.float32, smallest / len(cuts), high / len(cuts)))
        level = level * jnp.repeat(heights, shape[axis_at] // parts).reshape([-1 if axis == axis_at else 1 for axis in range(len(shape))])
    return level


def noise(own_key, shape, spread, most, shards=(), kind=jnp.bfloat16):
    factor_of = shard_levels(own_key, shape, shards, -0.22, 0.18) if shards else 1.0
    entries = jax.random.normal(own_key, shape, jnp.float32) * spread * factor_of
    return jnp.minimum(jnp.maximum(entries, -most), most).astype(kind)


def setup_inputs(seed: int = 0, part: int = 0) -> dict:
    key_list = jax.random.split(jax.random.key(seed), 7)
    part_splits = jax.random.split(jax.random.fold_in(key_list[6], part), 7)
    return {
        "acts": noise(part_splits[0], (TOK, D), 1.0, 6.0, ((0, 16), (1, 8))),
        "q_src": noise(part_splits[1], (D, QH * HD), D ** -0.5, 0.046875, ((0, 8), (1, 16))),
        "kv_src": noise(part_splits[2], (D, 2 * KVH * HD), D ** -0.5, 0.046875, ((0, 8), (1, 16))),
        "q_src_heads": draw_q_src_heads(jax.random.fold_in(key_list[6], 71), part),
        "q_tgt_heads": draw_q_tgt_heads(jax.random.fold_in(key_list[6], 71), part),
        "kv_tgt_heads": draw_kv_tgt_heads(jax.random.fold_in(key_list[6], 71), part),
    }


def reference(acts, q_src, kv_src, q_src_heads, q_tgt_heads, kv_tgt_heads):
    head_ids = jnp.arange(QH, dtype=jnp.int32)
    matches = (q_src_heads[None, :] == q_tgt_heads[:, None]).astype(jnp.int32)
    slot_of = jnp.sum(matches * head_ids[None, :], axis=1).astype(jnp.int32)
    q_three = q_src.reshape(D, QH, HD)
    q_new = jnp.take(q_three, slot_of, axis=1).reshape(D, QH * HD)
    kv_three = kv_src.reshape(D, KVH, 2 * HD)
    kv_new = jnp.take(kv_three, kv_tgt_heads, axis=1).reshape(D, 4 * KVH * HD)
    joined_cols = jnp.concatenate([q_new.reshape(D, N_TP, QDEV * HD), kv_new.reshape(D, N_TP, KVT * 2 * HD)], axis=2)
    joined_cols = joined_cols.reshape(D, N_TP * CDEV)
    qkv = jnp.dot(acts, joined_cols, preferred_element_type=jnp.float32).astype(jnp.bfloat16)
    return q_new, kv_new, qkv
```

```python
import functools

import jax
import jax.numpy as jnp
from jax import lax
from jax.experimental import pallas as pl
from jax.experimental.pallas import tpu as pltpu
from jax.sharding import PartitionSpec as P

HD = 128
F32, BF16 = jnp.float32, jnp.bfloat16
FILL = 16


def distances(tp, heads):
    capacity = max(2, heads // tp)
    select = heads // capacity
    stride = tp // select
    return [min(1, stride - 1)] + [k * stride for k in range(1, select)], capacity, stride


def mul(index, size):
    return pl.multiple_of(index * size, size)


def exchange(tp, subs, sel_ref, kvt_ref, acts_ref, q_ref, kv_ref, qraw, kvraw, sraw, kvres,
             acts, qv, sendq, kvbuf, kvsend, part, rsbuf, res, ssel, ld, asend, arecv, apsend, aprecv,
             ksend, krecv, kpsend, kprecv, qsend, qrecv, fsend, frecv, rsend, rrecv, ss_send, ss_recv):
    t, x = lax.axis_index("tp"), lax.axis_index("sub")
    core, y = lax.rem(t, 2), t // 2
    ring = tp // 2
    full = ring // 2 - 1
    toks, rows = acts_ref.shape[0], q_ref.shape[0]
    heads = q_ref.shape[1] // HD
    dist, cap, _ = distances(tp, heads)
    mate = t + 1 - 2 * core

    def at(d):
        return lax.rem(t + d + tp, tp)

    def remote(src, dst, send, recv, **where):
        copy = pltpu.make_async_remote_copy(
            src_ref=src, dst_ref=dst, send_sem=send, recv_sem=recv, device_id=where)
        copy.start()
        return copy

    def rows_of(index, first=0, count=toks):
        return acts.at[pl.ds(mul(index, toks) + first, count)]

    loads = [
        pltpu.make_async_copy(acts_ref, rows_of(t), ld.at[0]),
        pltpu.make_async_copy(kv_ref, kvbuf.at[y], ld.at[1]),
    ] + [pltpu.make_async_copy(q_ref.at[:, pl.ds(i * HD, HD)], qv.at[i], ld.at[2 + i]) for i in range(heads)]
    for copy in loads:
        copy.start()
    barrier = pltpu.get_barrier_semaphore()
    peers = {1, tp - 1, 2, tp - 2} | set(dist) | {tp - d for d in dist}
    for d in sorted(peers):
        pl.semaphore_signal(barrier, inc=1, device_id={"tp": at(d)})
    for d in (1, subs - 1):
        pl.semaphore_signal(barrier, inc=1, device_id={"sub": lax.rem(x + d, subs)})
    for copy in loads:
        copy.wait()
    for i in range(heads):
        sendq[i] = qv[sel_ref[i]]
    pl.semaphore_wait(barrier, len(peers) + 2)

    sent = []
    for d in (0, 1):
        sent.append(remote(rows_of(t), rows_of(t), asend.at[d, 0], arecv.at[d, 0], tp=at(2 - 4 * d)))
    sent.append(remote(rows_of(t), rows_of(t), apsend.at[0], aprecv.at[0], tp=mate))
    fills = []
    far = len(dist) // 2
    per_head = FILL // cap
    span = rows // per_head

    def fill(count):
        for _ in range(count):
            i = len(fills)
            if i == FILL:
                return
            head, piece = far * cap + i % cap, i // cap
            cut = pl.ds(piece * span, span)
            fills.append(remote(sendq.at[head, cut], qraw.at[head, cut], fsend.at[i], frecv.at[i], tp=at(dist[far])))

    fill(1)
    half = toks // 2
    for step in range(1, full + 2):
        for d in (0, 1):
            origin = at(-2 * step) if d == 0 else at(2 * step)
            if step <= full:
                block = rows_of(origin)
            else:
                block = rows_of(origin, d * half, half)
            pltpu.make_async_remote_copy(
                src_ref=block, dst_ref=block, send_sem=asend.at[d, step - 1], recv_sem=arecv.at[d, step - 1],
                device_id={"tp": t}).wait_recv()
            if step < full:
                sent.append(remote(block, block, asend.at[d, step], arecv.at[d, step], tp=at(2 - 4 * d)))
            elif step == full:
                block = rows_of(origin, d * half, half)
                sent.append(remote(block, block, asend.at[d, step], arecv.at[d, step], tp=at(2 - 4 * d)))
            if step <= full:
                block = rows_of(origin)
                k = 2 * step - 1 + d
                sent.append(remote(block, block, apsend.at[k], aprecv.at[k], tp=mate))
        if step == 1:
            for d in (0, 1):
                sent.append(remote(kvbuf.at[y], kvbuf.at[y], ksend.at[d, 0], krecv.at[d, 0], tp=at(2 - 4 * d)))
        fill(1)
    last = 2 * full + 1
    block = rows_of(at(ring))
    sent.append(remote(block, block, apsend.at[last], aprecv.at[last], tp=mate))

    def landed(k):
        step, d = (k + 1) // 2, (k + 1) % 2
        origin = t if k == 0 else (at(-2 * step) if d == 0 else at(2 * step))
        if k == last:
            origin = at(ring)
        other = origin + 1 - 2 * core
        block = rows_of(other)
        pltpu.make_async_remote_copy(
            src_ref=block, dst_ref=block, send_sem=apsend.at[k], recv_sem=aprecv.at[k], device_id={"tp": t}).wait_recv()

    for k in range(last + 1):
        landed(k)

    tile = 256

    def product(j, rhs):
        @pl.loop(0, acts.shape[0] // tile)
        def _(m):
            r = pl.ds(mul(m, tile), tile)
            p = jnp.dot(acts[r, :], rhs(), preferred_element_type=F32)
            part[j, 0, r, :] = p[:, :HD]
            part[j, 1, r, :] = p[:, HD:]

    pairs = heads // 2
    todo = list(range(pairs))
    for step in range(1, full + 2):
        for d in (0, 1):
            steps = full + d
            if step > steps:
                continue
            origin = lax.rem(y - step + ring, ring) if d == 0 else lax.rem(y + step, ring)
            block = kvbuf.at[origin]
            pltpu.make_async_remote_copy(
                src_ref=block, dst_ref=block, send_sem=ksend.at[d, step - 1], recv_sem=krecv.at[d, step - 1],
                device_id={"tp": t}).wait_recv()
            if step < steps:
                sent.append(remote(block, block, ksend.at[d, step], krecv.at[d, step], tp=at(2 - 4 * d)))
        fill(2)
        if todo:
            j = todo.pop(0)
            product(j, lambda j=j: jnp.concatenate([qv[2 * j], qv[2 * j + 1]], axis=1))
    for j in todo:
        product(j, lambda j=j: jnp.concatenate([qv[2 * j], qv[2 * j + 1]], axis=1))
    fill(FILL)
    near = [k for k in range(len(dist)) if k not in (far, 0)] + [0]
    order = [(k, r) for r in range(cap) for k in near[:-1]] + [(0, r) for r in range(cap)]
    for k, r in order:
        i = k * cap + r
        sent.append(remote(sendq.at[i], qraw.at[i], qsend.at[i], qrecv.at[i], tp=at(dist[k])))

    kvraw[core] = kvbuf[kvt_ref[t]]
    kvsend[...] = kvbuf[kvt_ref[mate]]
    sent.append(remote(kvsend, kvraw.at[core], kpsend, kprecv, tp=mate))

    def rs_copy(j, d, s):
        b = lax.rem(x - 1 - s + 2 * subs, subs) if d == 0 else lax.rem(x + 1 + s, subs)
        block = part.shape[2] // subs
        return pltpu.make_async_remote_copy(
            src_ref=part.at[j, d, pl.ds(mul(b, block), block)], dst_ref=rsbuf.at[j, d, s],
            send_sem=rsend.at[j, d, s], recv_sem=rrecv.at[j, d, s],
            device_id={"sub": lax.rem(x + (1 if d == 0 else subs - 1), subs)})

    def rs_add(j, d, s):
        b = lax.rem(x - 2 - s + 2 * subs, subs) if d == 0 else lax.rem(x + 2 + s, subs)
        block = part.shape[2] // subs
        rs_copy(j, d, s).wait_recv()
        r = pl.ds(mul(b, block), block)
        part[j, d, r, :] += rsbuf[j, d, s]

    streams = [(j, d) for j in range(pairs + 1) for d in (0, 1)]
    for j, d in streams[:-2]:
        rs_copy(j, d, 0).start()
    pltpu.make_async_remote_copy(
        src_ref=kvsend, dst_ref=kvraw.at[1 - core], send_sem=kpsend, recv_sem=kprecv, device_id={"tp": t}).wait_recv()
    product(pairs, lambda: jnp.concatenate([kvraw[0], kvraw[1]], axis=1))
    for j, d in streams[-2:]:
        rs_copy(j, d, 0).start()

    @pl.loop(0, subs - 2)
    def _(s):
        ready = None
        for j, d in streams:
            rs_add(j, d, s)
            if ready is not None:
                rs_copy(*ready, s + 1).start()
            ready = (j, d)
        rs_copy(*ready, s + 1).start()

    mine = pl.ds(mul(x, part.shape[2] // subs), part.shape[2] // subs)
    for j, d in streams:
        rs_add(j, d, subs - 2)
        if j < pairs:
            res[2 * j + d] = part[j, d, mine, :].astype(BF16)
        else:
            kvres[d] = part[j, d, mine, :].astype(BF16)
    for i in range(heads):
        ssel[i] = res[sel_ref[i]]
    for i in range(heads):
        sent.append(remote(ssel.at[i], sraw.at[i], ss_send.at[i], ss_recv.at[i], tp=at(dist[i // cap])))

    @pl.loop(0, subs - 1)
    def _(s):
        for j, d in streams:
            rs_copy(j, d, s).wait_send()

    for copy in sent:
        copy.wait_send()
    for copy in fills:
        copy.wait()
    for k, r in order:
        i = k * cap + r
        pltpu.make_async_remote_copy(
            src_ref=sendq.at[i], dst_ref=qraw.at[i], send_sem=qsend.at[i], recv_sem=qrecv.at[i], device_id={"tp": t}).wait_recv()
    for i in range(heads):
        pltpu.make_async_remote_copy(
            src_ref=ssel.at[i], dst_ref=sraw.at[i], send_sem=ss_send.at[i], recv_sem=ss_recv.at[i], device_id={"tp": t}).wait_recv()


def place(gat, qraw, kvraw, sraw, kvres, q_new, kv_new, qkv, sem):
    heads = qraw.shape[0]
    copies = []
    for p in range(heads):
        cols = pl.ds(p * HD, HD)
        copies.append(pltpu.make_async_copy(qraw.at[gat[p]], q_new.at[:, cols], sem.at[0, p]))
        copies.append(pltpu.make_async_copy(sraw.at[gat[p]], qkv.at[:, cols], sem.at[1, p]))
    for p in range(2):
        copies.append(pltpu.make_async_copy(kvraw.at[p], kv_new.at[:, pl.ds(p * HD, HD)], sem.at[2, p]))
        copies.append(pltpu.make_async_copy(kvres.at[p], qkv.at[:, pl.ds((heads + p) * HD, HD)], sem.at[3, p]))
    for copy in copies:
        copy.start()
    for copy in copies:
        copy.wait()


def per_device(tp, subs, acts, q_src, kv_src, q_src_heads, q_tgt_heads, kv_tgt_heads):
    t = lax.axis_index("tp")
    toks, depth = acts.shape
    rows, heads = q_src.shape[0], q_src.shape[1] // HD
    dist, cap, stride = distances(tp, heads)
    own = jnp.arange(heads, dtype=jnp.int32)
    ids = jnp.arange(heads * tp, dtype=jnp.int32)

    def slot(block, other):
        held = lax.dynamic_slice_in_dim(block, t * heads, heads)
        return jnp.sum(jnp.where(held[:, None] == other[None, :], ids[None, :], 0), axis=1)

    def hop(d):
        return jnp.where(d % stride == 0, d // stride, 0)

    to = hop((slot(q_src_heads, q_tgt_heads) // heads - t) % tp)
    rank = jnp.sum((to[:, None] == to[None, :]) & (own[None, :] < own[:, None]), axis=1, dtype=jnp.int32)
    sel = jnp.sum(jnp.where((to * cap + rank)[None, :] == own[:, None], own[None, :], 0), axis=1, dtype=jnp.int32)
    pos = slot(q_tgt_heads, q_src_heads)
    come = hop((t - pos // heads) % tp)
    order = jnp.sum((come[:, None] == come[None, :]) & (pos[None, :] < pos[:, None]), axis=1, dtype=jnp.int32)
    gat = come * cap + order

    wide = rows, HD
    tokens = toks * tp
    block = tokens // subs
    ring = tp // 2
    full = ring // 2 - 1
    dma = pltpu.SemaphoreType.DMA
    vmem = pl.BlockSpec(memory_space=pltpu.VMEM)
    smem = pl.BlockSpec(memory_space=pltpu.SMEM)
    anyp = pl.BlockSpec(memory_space=pl.ANY)
    raw = pl.pallas_call(
        functools.partial(exchange, tp, subs),
        out_shape=(
            pltpu.VMEM((heads, *wide), BF16),
            pltpu.VMEM((2, *wide), BF16),
            pltpu.VMEM((heads, block, HD), BF16),
            pltpu.VMEM((2, block, HD), BF16),
        ),
        in_specs=[smem, smem, anyp, anyp, anyp],
        out_specs=(vmem, vmem, vmem, vmem),
        scratch_shapes=[
            pltpu.VMEM((tokens, depth), BF16),
            pltpu.VMEM((heads, *wide), BF16),
            pltpu.VMEM((heads, *wide), BF16),
            pltpu.VMEM((ring, *wide), BF16),
            pltpu.VMEM(wide, BF16),
            pltpu.VMEM((heads // 2 + 1, 2, tokens, HD), F32),
            pltpu.VMEM((heads // 2 + 1, 2, subs - 1, block, HD), F32),
            pltpu.VMEM((heads, block, HD), BF16),
            pltpu.VMEM((heads, block, HD), BF16),
            dma((2 + heads,)),
            dma((2, full + 1)),
            dma((2, full + 1)),
            dma((ring,)),
            dma((ring,)),
            dma((2, full + 1)),
            dma((2, full + 1)),
            dma,
            dma,
            dma((heads,)),
            dma((heads,)),
            dma((FILL,)),
            dma((FILL,)),
            dma((heads // 2 + 1, 2, subs - 1)),
            dma((heads // 2 + 1, 2, subs - 1)),
            dma((heads,)),
            dma((heads,)),
        ],
        compiler_params=pltpu.CompilerParams(
            collective_id=0, has_side_effects=True, vmem_limit_bytes=50 * 2**20),
        name="exchange",
    )(sel, kv_tgt_heads, acts, q_src, kv_src)
    return pl.pallas_call(
        place,
        out_shape=(
            jax.ShapeDtypeStruct(q_src.shape, BF16),
            jax.ShapeDtypeStruct((rows, 2 * HD), BF16),
            jax.ShapeDtypeStruct((block, (heads + 2) * HD), BF16),
        ),
        in_specs=[smem, anyp, anyp, anyp, anyp],
        out_specs=(anyp, anyp, anyp),
        scratch_shapes=[dma((4, heads))],
        compiler_params=pltpu.CompilerParams(vmem_limit_bytes=2**20),
        name="place",
    )(gat, *(pltpu.with_memory_space_constraint(a, pltpu.VMEM) for a in raw))


def solution(mesh):
    in_specs = (
        P(("rep", "tp"), "sub"),
        P(("rep", "sub"), "tp"),
        P(("rep", "sub"), "tp"),
        P(),
        P(),
        P(),
    )
    out_specs = (P(("rep", "sub"), "tp"), P(("rep", "sub"), "tp"), P(("rep", "sub"), "tp"))
    return jax.shard_map(
        functools.partial(per_device, mesh.shape["tp"], mesh.shape["sub"]),
        mesh=mesh, in_specs=in_specs, out_specs=out_specs, check_vma=False)
```

```python
import functools

import jax
import jax.numpy as jnp
from jax import lax
from jax.experimental import pallas as pl
from jax.experimental.pallas import tpu as pltpu
from jax.sharding import PartitionSpec as P

HD = 128
F32, BF16 = jnp.float32, jnp.bfloat16
FILL = 16


def distances(tp, heads):
    capacity = max(2, heads // tp)
    select = heads // capacity
    stride = tp // select
    return [min(1, stride - 1)] + [k * stride for k in range(1, select)], capacity, stride


def routes(tp, t, heads, mine_ref, other_ref, out):
    _, cap, stride = distances(tp, heads)
    wanted = [mine_ref[t * heads + i] for i in range(heads)]

    def look(p, found):
        head = other_ref[p]
        return tuple(jnp.where(head == w, p, f) for w, f in zip(wanted, found))

    at = lax.fori_loop(0, heads * tp, look, (jnp.int32(0),) * heads, unroll=8)
    hops = []
    for pos in at:
        d = lax.rem(pos // heads - t + tp, tp)
        d = d if out else lax.rem(tp - d, tp)
        hops.append(jnp.where(lax.rem(d, stride) == 0, d // stride, 0))
    first = list(range(heads)) if out else at
    ranks = []
    for i in range(heads):
        before = [jnp.where((hops[j] == hops[i]) & (first[j] < first[i]), 1, 0) for j in range(heads) if j != i]
        ranks.append(hops[i] * cap + sum(before))
    return ranks


def mul(index, size):
    return pl.multiple_of(index * size, size)


def exchange(tp, subs, src_ref, tgt_ref, kvt_ref, acts_ref, q_ref, kv_ref, qraw, kvraw, sraw, kvres, gat,
             acts, qv, sendq, kvbuf, kvsend, part, rsbuf, res, ld, asend, arecv, apsend, aprecv,
             ksend, krecv, kpsend, kprecv, qsend, qrecv, fsend, frecv, rsend, rrecv, ss_send, ss_recv):
    t, x = lax.axis_index("tp"), lax.axis_index("sub")
    core, y = lax.rem(t, 2), t // 2
    ring = tp // 2
    full = ring // 2 - 1
    toks, rows = acts_ref.shape[0], q_ref.shape[0]
    heads = q_ref.shape[1] // HD
    dist, cap, _ = distances(tp, heads)
    mate = t + 1 - 2 * core

    def at(d):
        return lax.rem(t + d + tp, tp)

    def remote(src, dst, send, recv, **where):
        copy = pltpu.make_async_remote_copy(
            src_ref=src, dst_ref=dst, send_sem=send, recv_sem=recv, device_id=where)
        copy.start()
        return copy

    def rows_of(index, first=0, count=toks):
        return acts.at[pl.ds(mul(index, toks) + first, count)]

    loads = [
        pltpu.make_async_copy(acts_ref, rows_of(t), ld.at[0]),
        pltpu.make_async_copy(kv_ref, kvbuf.at[y], ld.at[1]),
    ] + [pltpu.make_async_copy(q_ref.at[:, pl.ds(i * HD, HD)], qv.at[i], ld.at[2 + i]) for i in range(heads)]
    for copy in loads:
        copy.start()
    barrier = pltpu.get_barrier_semaphore()
    peers = {1, tp - 1, 2, tp - 2} | set(dist) | {tp - d for d in dist}
    for d in sorted(peers):
        pl.semaphore_signal(barrier, inc=1, device_id={"tp": at(d)})
    for d in (1, subs - 1):
        pl.semaphore_signal(barrier, inc=1, device_id={"sub": lax.rem(x + d, subs)})
    for copy in loads[:2]:
        copy.wait()
    with jax.named_scope("barrier"):
        pl.semaphore_wait(barrier, len(peers) + 2)

    sent = []
    for d in (0, 1):
        sent.append(remote(rows_of(t), rows_of(t), asend.at[d, 0], arecv.at[d, 0], tp=at(2 - 4 * d)))
    sent.append(remote(rows_of(t), rows_of(t), apsend.at[0], aprecv.at[0], tp=mate))
    fills = []
    far = len(dist) // 2
    per_head = FILL // cap
    span = rows // per_head

    def fill(count):
        for _ in range(count):
            i = len(fills)
            if i == FILL:
                return
            head, piece = far * cap + i % cap, i // cap
            cut = pl.ds(piece * span, span)
            fills.append(remote(sendq.at[head, cut], qraw.at[head, cut], fsend.at[i], frecv.at[i], tp=at(dist[far])))

    place_of = routes(tp, t, heads, src_ref, tgt_ref, True)
    picks = [sum(jnp.where(r == i, slot, 0) for slot, r in enumerate(place_of)) for i in range(heads)]
    for copy in loads[2:]:
        copy.wait()
    with jax.named_scope("select"):
        for i in range(heads):
            sendq[i] = qv[picks[i]]
    fill(2)
    half = toks // 2
    for step in range(1, full + 2):
        for d in (0, 1):
            origin = at(-2 * step) if d == 0 else at(2 * step)
            if step <= full:
                block = rows_of(origin)
            else:
                block = rows_of(origin, d * half, half)
            with jax.named_scope(f"tokens{step}{d}"):
                pltpu.make_async_remote_copy(
                    src_ref=block, dst_ref=block, send_sem=asend.at[d, step - 1], recv_sem=arecv.at[d, step - 1],
                    device_id={"tp": t}).wait_recv()
            if step < full:
                sent.append(remote(block, block, asend.at[d, step], arecv.at[d, step], tp=at(2 - 4 * d)))
            elif step == full:
                block = rows_of(origin, d * half, half)
                sent.append(remote(block, block, asend.at[d, step], arecv.at[d, step], tp=at(2 - 4 * d)))
            if step <= full:
                block = rows_of(origin)
                k = 2 * step - 1 + d
                sent.append(remote(block, block, apsend.at[k], aprecv.at[k], tp=mate))
        if step == 1:
            for d in (0, 1):
                sent.append(remote(kvbuf.at[y], kvbuf.at[y], ksend.at[d, 0], krecv.at[d, 0], tp=at(2 - 4 * d)))
        fill(2)
    last = 2 * full + 1
    block = rows_of(at(ring))
    sent.append(remote(block, block, apsend.at[last], aprecv.at[last], tp=mate))

    def landed(k):
        step, d = (k + 1) // 2, (k + 1) % 2
        origin = t if k == 0 else (at(-2 * step) if d == 0 else at(2 * step))
        if k == last:
            origin = at(ring)
        other = origin + 1 - 2 * core
        block = rows_of(other)
        pltpu.make_async_remote_copy(
            src_ref=block, dst_ref=block, send_sem=apsend.at[k], recv_sem=aprecv.at[k], device_id={"tp": t}).wait_recv()

    with jax.named_scope("mate"):
        for k in range(last + 1):
            landed(k)

    tile = 256

    def product(j, rhs):
        @pl.loop(0, acts.shape[0] // tile)
        def _(m):
            r = pl.ds(mul(m, tile), tile)
            p = jnp.dot(acts[r, :], rhs(), preferred_element_type=F32)
            part[j, 0, r, :] = p[:, :HD]
            part[j, 1, r, :] = p[:, HD:]

    pairs = heads // 2
    todo = [j for j in range(pairs) if j != far]

    def rs_copy(j, d, s):
        b = lax.rem(x - 1 - s + 2 * subs, subs) if d == 0 else lax.rem(x + 1 + s, subs)
        block = part.shape[2] // subs
        return pltpu.make_async_remote_copy(
            src_ref=part.at[j, d, pl.ds(mul(b, block), block)], dst_ref=rsbuf.at[j, d, s],
            send_sem=rsend.at[j, d, s], recv_sem=rrecv.at[j, d, s],
            device_id={"sub": lax.rem(x + (1 if d == 0 else subs - 1), subs)})

    def rs_add(j, d, s):
        b = lax.rem(x - 2 - s + 2 * subs, subs) if d == 0 else lax.rem(x + 2 + s, subs)
        block = part.shape[2] // subs
        rs_copy(j, d, s).wait_recv()
        r = pl.ds(mul(b, block), block)
        part[j, d, r, :] += rsbuf[j, d, s]

    def pair(ref, j):
        return jnp.concatenate([ref[2 * j], ref[2 * j + 1]], axis=1)

    def here(j):
        with jax.named_scope(f"product{j}"):
            product(j, lambda: pair(sendq, j))
        for d in (0, 1):
            rs_copy(j, d, 0).start()

    def rs_step(streams, s):
        with jax.named_scope(f"reduce{s}"):
            ready = None
            for j, d in streams:
                rs_add(j, d, s)
                if s == subs - 2:
                    total = part[j, d, mine, :].astype(BF16)
                    if j == pairs:
                        kvres[d] = total
                    elif j == far:
                        sraw[2 * j + d] = total
                    else:
                        res[2 * j + d] = total
                    continue
                if ready is not None:
                    rs_copy(*ready, s + 1).start()
                ready = (j, d)
            if ready is not None:
                rs_copy(*ready, s + 1).start()

    mine = pl.ds(mul(x, part.shape[2] // subs), part.shape[2] // subs)
    early = [(j, d) for j in todo for d in (0, 1)]
    late = [(j, d) for j in (pairs, far) for d in (0, 1)]

    def straight(k):
        for r in range(cap):
            i = k * cap + r
            sent.append(remote(sendq.at[i], qraw.at[i], qsend.at[i], qrecv.at[i], tp=at(dist[k])))

    near = [k for k in range(1, len(dist)) if k != far]
    done = 0
    for step in range(1, full + 2):
        for d in (0, 1):
            steps = full + d
            if step > steps:
                continue
            origin = lax.rem(y - step + ring, ring) if d == 0 else lax.rem(y + step, ring)
            block = kvbuf.at[origin]
            with jax.named_scope(f"kv{step}{d}"):
                pltpu.make_async_remote_copy(
                    src_ref=block, dst_ref=block, send_sem=ksend.at[d, step - 1], recv_sem=krecv.at[d, step - 1],
                    device_id={"tp": t}).wait_recv()
            if step < steps:
                sent.append(remote(block, block, ksend.at[d, step], krecv.at[d, step], tp=at(2 - 4 * d)))
        fill(2)
        if step == full:
            straight(0)
        if step == 1:
            for j in todo:
                here(j)
        elif step <= full:
            for _ in range(2):
                rs_step(early, done)
                done += 1
    fill(FILL)
    for k in near:
        straight(k)
    kvraw[core] = kvbuf[kvt_ref[t]]
    kvsend[...] = kvbuf[kvt_ref[mate]]
    sent.append(remote(kvsend, kvraw.at[core], kpsend, kprecv, tp=mate))
    rs_step(early, done)
    pltpu.make_async_remote_copy(
        src_ref=kvsend, dst_ref=kvraw.at[1 - core], send_sem=kpsend, recv_sem=kprecv, device_id={"tp": t}).wait_recv()
    product(pairs, lambda: pair(kvraw, 0))
    for d in (0, 1):
        rs_copy(pairs, d, 0).start()
    for s in range(done + 1, subs - 1):
        rs_step(early, s)
    back = [i for i in range(heads) if i // cap != far]
    for i in back:
        sent.append(remote(res.at[i], sraw.at[i], ss_send.at[i], ss_recv.at[i], tp=at(dist[i // cap])))
    for i, r in enumerate(routes(tp, t, heads, tgt_ref, src_ref, False)):
        gat[i] = r
    with jax.named_scope("far"):
        for copy in fills:
            copy.wait_recv()
    product(far, lambda: pair(qraw, far))
    for d in (0, 1):
        rs_copy(far, d, 0).start()
    for s in range(subs - 1):
        rs_step(late, s)

    @pl.loop(0, subs - 1)
    def _(s):
        for j, d in early + late:
            rs_copy(j, d, s).wait_send()

    with jax.named_scope("sent"):
        for copy in sent:
            copy.wait_send()
    for copy in fills:
        copy.wait_send()
    for i in back:
        with jax.named_scope(f"head{i}"):
            pltpu.make_async_remote_copy(
                src_ref=sendq.at[i], dst_ref=qraw.at[i], send_sem=qsend.at[i], recv_sem=qrecv.at[i], device_id={"tp": t}).wait_recv()
    with jax.named_scope("back"):
        for i in back:
            pltpu.make_async_remote_copy(
                src_ref=res.at[i], dst_ref=sraw.at[i], send_sem=ss_send.at[i], recv_sem=ss_recv.at[i], device_id={"tp": t}).wait_recv()


def place(gat, qraw, kvraw, sraw, kvres, q_new, kv_new, qkv, sem):
    heads = qraw.shape[0]
    copies = []
    for p in range(heads):
        cols = pl.ds(p * HD, HD)
        copies.append(pltpu.make_async_copy(qraw.at[gat[p]], q_new.at[:, cols], sem.at[0, p]))
        copies.append(pltpu.make_async_copy(sraw.at[gat[p]], qkv.at[:, cols], sem.at[1, p]))
    for p in range(2):
        copies.append(pltpu.make_async_copy(kvraw.at[p], kv_new.at[:, pl.ds(p * HD, HD)], sem.at[2, p]))
        copies.append(pltpu.make_async_copy(kvres.at[p], qkv.at[:, pl.ds((heads + p) * HD, HD)], sem.at[3, p]))
    for copy in copies:
        copy.start()
    for copy in copies:
        copy.wait()


def per_device(tp, subs, acts, q_src, kv_src, q_src_heads, q_tgt_heads, kv_tgt_heads):
    toks, depth = acts.shape
    rows, heads = q_src.shape[0], q_src.shape[1] // HD
    wide = rows, HD
    tokens = toks * tp
    block = tokens // subs
    ring = tp // 2
    full = ring // 2 - 1
    dma = pltpu.SemaphoreType.DMA
    vmem = pl.BlockSpec(memory_space=pltpu.VMEM)
    smem = pl.BlockSpec(memory_space=pltpu.SMEM)
    anyp = pl.BlockSpec(memory_space=pl.ANY)
    *raw, gat = pl.pallas_call(
        functools.partial(exchange, tp, subs),
        out_shape=(
            pltpu.VMEM((heads, *wide), BF16),
            pltpu.VMEM((2, *wide), BF16),
            pltpu.VMEM((heads, block, HD), BF16),
            pltpu.VMEM((2, block, HD), BF16),
            jax.ShapeDtypeStruct((heads,), jnp.int32),
        ),
        in_specs=[smem, smem, smem, anyp, anyp, anyp],
        out_specs=(vmem, vmem, vmem, vmem, smem),
        scratch_shapes=[
            pltpu.VMEM((tokens, depth), BF16),
            pltpu.VMEM((heads, *wide), BF16),
            pltpu.VMEM((heads, *wide), BF16),
            pltpu.VMEM((ring, *wide), BF16),
            pltpu.VMEM(wide, BF16),
            pltpu.VMEM((heads // 2 + 1, 2, tokens, HD), F32),
            pltpu.VMEM((heads // 2 + 1, 2, subs - 1, block, HD), F32),
            pltpu.VMEM((heads, block, HD), BF16),
            dma((2 + heads,)),
            dma((2, full + 1)),
            dma((2, full + 1)),
            dma((ring,)),
            dma((ring,)),
            dma((2, full + 1)),
            dma((2, full + 1)),
            dma,
            dma,
            dma((heads,)),
            dma((heads,)),
            dma((FILL,)),
            dma((FILL,)),
            dma((heads // 2 + 1, 2, subs - 1)),
            dma((heads // 2 + 1, 2, subs - 1)),
            dma((heads,)),
            dma((heads,)),
        ],
        compiler_params=pltpu.CompilerParams(
            collective_id=0, has_side_effects=True, vmem_limit_bytes=50 * 2**20),
        name="exchange",
    )(q_src_heads, q_tgt_heads, kv_tgt_heads, acts, q_src, kv_src)
    return pl.pallas_call(
        place,
        out_shape=(
            jax.ShapeDtypeStruct(q_src.shape, BF16),
            jax.ShapeDtypeStruct((rows, 2 * HD), BF16),
            jax.ShapeDtypeStruct((block, (heads + 2) * HD), BF16),
        ),
        in_specs=[smem, anyp, anyp, anyp, anyp],
        out_specs=(anyp, anyp, anyp),
        scratch_shapes=[dma((4, heads))],
        compiler_params=pltpu.CompilerParams(vmem_limit_bytes=2**20),
        name="place",
    )(gat, *(pltpu.with_memory_space_constraint(a, pltpu.VMEM) for a in raw))


def solution(mesh):
    in_specs = (
        P(("rep", "tp"), "sub"),
        P(("rep", "sub"), "tp"),
        P(("rep", "sub"), "tp"),
        P(),
        P(),
        P(),
    )
    out_specs = (P(("rep", "sub"), "tp"), P(("rep", "sub"), "tp"), P(("rep", "sub"), "tp"))
    return jax.shard_map(
        functools.partial(per_device, mesh.shape["tp"], mesh.shape["sub"]),
        mesh=mesh, in_specs=in_specs, out_specs=out_specs, check_vma=False)
```

```python
import functools

import jax
import jax.numpy as jnp
from jax import lax
from jax.experimental import pallas as pl
from jax.experimental.pallas import tpu as pltpu
from jax.sharding import PartitionSpec as P

HD = 128
F32, BF16 = jnp.float32, jnp.bfloat16
FILL = 16
FILL0, FILL1 = 2, 4
Q1 = 3
LEG = 2


def distances(tp, heads):
    capacity = max(2, heads // tp)
    select = heads // capacity
    stride = tp // select
    return [min(1, stride - 1)] + [k * stride for k in range(1, select)], capacity, stride


def routes(tp, t, heads, mine_ref, other_ref, out):
    _, cap, stride = distances(tp, heads)
    wanted = [mine_ref[t * heads + i] for i in range(heads)]

    def look(p, found):
        head = other_ref[p]
        return tuple(jnp.where(head == w, p, f) for w, f in zip(wanted, found))

    at = lax.fori_loop(0, heads * tp, look, (jnp.int32(0),) * heads, unroll=8)
    hops = []
    for pos in at:
        d = lax.rem(pos // heads - t + tp, tp)
        d = d if out else lax.rem(tp - d, tp)
        hops.append(jnp.where(lax.rem(d, stride) == 0, d // stride, 0))
    first = list(range(heads)) if out else at
    ranks = []
    for i in range(heads):
        before = [jnp.where((hops[j] == hops[i]) & (first[j] < first[i]), 1, 0) for j in range(heads) if j != i]
        ranks.append(hops[i] * cap + sum(before))
    return ranks


def mul(index, size):
    return pl.multiple_of(index * size, size)


def exchange(tp, subs, src_ref, tgt_ref, kvt_ref, acts_ref, q_ref, kv_ref, qraw, kvraw, sraw, kvres, gat_ref,
             gat, acts, qv, sendq, kvown, kvbuf, kvsend, part, rsbuf, res, ld, asend, arecv, apsend, aprecv,
             k1send, k1recv, k2send, k2recv, qsend, qrecv, rsend, rrecv, ss_send, ss_recv):
    t, x = lax.axis_index("tp"), lax.axis_index("sub")
    core, y = lax.rem(t, 2), t // 2
    ring = tp // 2
    full = ring // 2 - 1
    toks, rows = acts_ref.shape[0], q_ref.shape[0]
    heads = q_ref.shape[1] // HD
    pairs = heads // 2
    dist, cap, _ = distances(tp, heads)
    far = len(dist) // 2
    near = [k for k in range(1, len(dist)) if k != far]
    mate = t + 1 - 2 * core
    piece = rows // ring
    block = acts.shape[0] // subs

    def at(d):
        return lax.rem(t + d + 2 * tp, tp)

    def chip(d):
        return lax.rem(y + d + ring, ring)

    def describe(src, dst, send, recv, **where):
        return pltpu.make_async_remote_copy(
            src_ref=src, dst_ref=dst, send_sem=send, recv_sem=recv, device_id=where)

    def remote(src, dst, send, recv, **where):
        describe(src, dst, send, recv, **where).start()

    def arrived(dst, send, recv):
        describe(dst, dst, send, recv, tp=t).wait_recv()

    def tokens_of(index):
        return acts.at[pl.ds(mul(index, toks), toks)]

    def rows_of(index):
        return pl.ds(mul(index, piece), piece)

    loads = [
        pltpu.make_async_copy(acts_ref, tokens_of(t), ld.at[0]),
        pltpu.make_async_copy(kv_ref, kvown, ld.at[1]),
        pltpu.make_async_copy(kv_ref.at[rows_of(y)], kvbuf.at[y], ld.at[2]),
    ] + [pltpu.make_async_copy(q_ref.at[:, pl.ds(i * HD, HD)], qv.at[i], ld.at[3]) for i in range(heads)]
    for copy in loads:
        copy.start()
    barrier = pltpu.get_barrier_semaphore()
    for d in range(1, tp):
        pl.semaphore_signal(barrier, inc=1, device_id={"tp": at(d)})
    for d in (1, subs - 1):
        pl.semaphore_signal(barrier, inc=1, device_id={"sub": lax.rem(x + d, subs)})
    for copy in loads[:3]:
        copy.wait()
    with jax.named_scope("barrier"):
        pl.semaphore_wait(barrier, tp + 1)

    def tokens(d, step, origin):
        remote(tokens_of(origin), tokens_of(origin), asend, arecv.at[d, step], tp=at(2 - 4 * d))

    def hand(origin):
        remote(tokens_of(origin), tokens_of(origin), apsend, aprecv, tp=mate)

    tokens(0, 0, t)
    tokens(1, 0, t)
    hand(t)
    for d in range(1, ring):
        remote(kvown.at[rows_of(chip(d))], kvbuf.at[y], k1send, k1recv, tp=at(2 * d))

    place_of = routes(tp, t, heads, src_ref, tgt_ref, True)
    picks = [sum(jnp.where(r == i, slot, 0) for slot, r in enumerate(place_of)) for i in range(heads)]
    pltpu.make_async_copy(qv, qv, ld.at[3]).wait()
    with jax.named_scope("select"):
        for i in range(heads):
            sendq[i] = qv[picks[i]]

    fills = []
    per_head = FILL // cap
    span = rows // per_head

    def fill(count):
        start = len(fills)
        for n in range(start, min(start + count, FILL)):
            fills.append(n)
            for f, k in enumerate(near):
                head, cut = k * cap + n // per_head, pl.ds(n % per_head * span, span)
                remote(sendq.at[head, cut], qraw.at[head, cut], qsend, qrecv, tp=at(dist[k]))

    def straight(k):
        for i in range(k * cap, (k + 1) * cap):
            remote(sendq.at[i], qraw.at[i], qsend, qrecv, tp=at(dist[k]))

    def second_leg():
        with jax.named_scope("leg1"):
            arrived(kvbuf.at[pl.ds(1, ring - 1)], k1send, k1recv)
        for d in range(1, tp):
            kvsend[d] = kvbuf[kvt_ref[at(d)]]
        kvraw[core, rows_of(y), :] = kvbuf[kvt_ref[t]]
        for d in sorted(range(1, tp), key=lambda d: -min(d, tp - d)):
            remote(kvsend.at[d], kvraw.at[core, rows_of(y)], k2send, k2recv, tp=at(d))

    fill(FILL0)
    for step in range(1, full + 2):
        for d in (0, 1):
            if step > full + d:
                continue
            origin = at(-2 * step) if d == 0 else at(2 * step)
            with jax.named_scope(f"tokens{step}{d}"):
                arrived(tokens_of(origin), asend, arecv.at[d, step - 1])
            if step < full + d:
                tokens(d, step, origin)
            hand(origin)
        if step == LEG:
            second_leg()
        fill(FILL1)
        if step == Q1:
            straight(0)

    tile = 256

    def product(j, ref, first):
        with jax.named_scope(f"product{j}"):
            @pl.loop(0, acts.shape[0] // tile)
            def _(m):
                r = pl.ds(mul(m, tile), tile)
                rhs = jnp.concatenate([ref[first], ref[first + 1]], axis=1)
                p = jnp.dot(acts[r, :], rhs, preferred_element_type=F32)
                part[j, 0, r, :] = p[:, :HD]
                part[j, 1, r, :] = p[:, HD:]
        for d in (0, 1):
            rs_copy(j, d, 0).start()

    def part_of(b):
        return pl.ds(mul(b, block), block)

    def rs_copy(j, d, s):
        b = lax.rem(x - 1 - s + 2 * subs, subs) if d == 0 else lax.rem(x + 1 + s, subs)
        return describe(part.at[j, d, part_of(b)], rsbuf.at[j, d, s], rsend.at[j, d], rrecv.at[j, d, s],
                        sub=lax.rem(x + (1 if d == 0 else subs - 1), subs))

    def rs_step(group, s):
        with jax.named_scope(f"reduce{s}"):
            ready = None
            for j in group:
                for d in (0, 1):
                    b = lax.rem(x - 2 - s + 2 * subs, subs) if d == 0 else lax.rem(x + 2 + s, subs)
                    rs_copy(j, d, s).wait_recv()
                    total = part[j, d, part_of(b), :] + rsbuf[j, d, s]
                    if s == subs - 2:
                        total = total.astype(BF16)
                        if j == pairs:
                            kvres[d] = total
                        else:
                            res[2 * j + d] = total
                        continue
                    part[j, d, part_of(b), :] = total
                    rs_copy(j, d, s).wait_send()
                    if ready is not None:
                        rs_copy(*ready, s + 1).start()
                    ready = (j, d)
            if ready is not None:
                rs_copy(*ready, s + 1).start()

    with jax.named_scope("mate"):
        arrived(acts.at[pl.ds(0, ring * toks)], apsend, aprecv)

    for k in range(pairs):
        product(k, sendq, k * cap)
    with jax.named_scope("leg2"):
        arrived(kvsend.at[pl.ds(1, tp - 1)], k2send, k2recv)
    product(pairs, kvraw, 0)
    fill(FILL)
    straight(far)
    group = list(range(pairs + 1))
    for s in range(subs - 1):
        rs_step(group, s)
    back = range(heads)
    for i in back:
        remote(res.at[i], sraw.at[i], ss_send, ss_recv, tp=at(dist[i // cap]))
    for i, r in enumerate(routes(tp, t, heads, tgt_ref, src_ref, False)):
        gat[i] = r
    table = pltpu.make_async_copy(gat, gat_ref, ld.at[0])
    table.start()
    for j in group:
        for d in (0, 1):
            rs_copy(j, d, subs - 2).wait_send()

    table.wait()
    with jax.named_scope("sent"):
        for src, sem in ((acts.at[pl.ds(0, (2 * full + 1) * toks)], asend), (acts.at[pl.ds(0, ring * toks)], apsend),
                         (kvbuf.at[pl.ds(1, ring - 1)], k1send), (kvsend.at[pl.ds(1, tp - 1)], k2send),
                         (sendq, qsend), (res, ss_send)):
            describe(src, src, sem, sem, tp=t).wait_send()
    with jax.named_scope("heads"):
        arrived(qraw, qsend, qrecv)
    with jax.named_scope("back"):
        arrived(sraw, ss_send, ss_recv)


def place(gat, qraw, kvraw, sraw, kvres, q_new, kv_new, qkv, sem):
    heads = qraw.shape[0]
    copies = []
    for p in range(heads):
        cols = pl.ds(p * HD, HD)
        copies.append(pltpu.make_async_copy(qraw.at[gat[p]], q_new.at[:, cols], sem.at[0, p]))
        copies.append(pltpu.make_async_copy(sraw.at[gat[p]], qkv.at[:, cols], sem.at[1, p]))
    for p in range(2):
        copies.append(pltpu.make_async_copy(kvraw.at[p], kv_new.at[:, pl.ds(p * HD, HD)], sem.at[2, p]))
        copies.append(pltpu.make_async_copy(kvres.at[p], qkv.at[:, pl.ds((heads + p) * HD, HD)], sem.at[3, p]))
    for copy in copies:
        copy.start()
    for copy in copies:
        copy.wait()


def per_device(tp, subs, acts, q_src, kv_src, q_src_heads, q_tgt_heads, kv_tgt_heads):
    toks, depth = acts.shape
    rows, heads = q_src.shape[0], q_src.shape[1] // HD
    dist, _, _ = distances(tp, heads)
    wide = rows, HD
    tokens = toks * tp
    block = tokens // subs
    ring = tp // 2
    full = ring // 2 - 1
    dma = pltpu.SemaphoreType.DMA
    vmem = pl.BlockSpec(memory_space=pltpu.VMEM)
    smem = pl.BlockSpec(memory_space=pltpu.SMEM)
    anyp = pl.BlockSpec(memory_space=pl.ANY)
    *raw, gat = pl.pallas_call(
        functools.partial(exchange, tp, subs),
        out_shape=(
            pltpu.VMEM((heads, *wide), BF16),
            pltpu.VMEM((2, *wide), BF16),
            pltpu.VMEM((heads, block, HD), BF16),
            pltpu.VMEM((2, block, HD), BF16),
            jax.ShapeDtypeStruct((heads,), jnp.int32),
        ),
        in_specs=[smem, smem, smem, anyp, anyp, anyp],
        out_specs=(vmem, vmem, vmem, vmem, anyp),
        scratch_shapes=[
            pltpu.SMEM((heads,), jnp.int32),
            pltpu.VMEM((tokens, depth), BF16),
            pltpu.VMEM((heads, *wide), BF16),
            pltpu.VMEM((heads, *wide), BF16),
            pltpu.VMEM(wide, BF16),
            pltpu.VMEM((ring, rows // ring, HD), BF16),
            pltpu.VMEM((tp, rows // ring, HD), BF16),
            pltpu.VMEM((heads // 2 + 1, 2, tokens, HD), F32),
            pltpu.VMEM((heads // 2 + 1, 2, subs - 1, block, HD), F32),
            pltpu.VMEM((heads, block, HD), BF16),
            dma((4,)),
            dma,
            dma((2, full + 1)),
            *[dma] * 8,
            dma((heads // 2 + 1, 2)),
            dma((heads // 2 + 1, 2, subs - 1)),
            dma,
            dma,
        ],
        compiler_params=pltpu.CompilerParams(
            collective_id=0, has_side_effects=True, vmem_limit_bytes=50 * 2**20),
        name="exchange",
    )(q_src_heads, q_tgt_heads, kv_tgt_heads, acts, q_src, kv_src)
    return pl.pallas_call(
        place,
        out_shape=(
            jax.ShapeDtypeStruct(q_src.shape, BF16),
            jax.ShapeDtypeStruct((rows, 2 * HD), BF16),
            jax.ShapeDtypeStruct((block, (heads + 2) * HD), BF16),
        ),
        in_specs=[smem, anyp, anyp, anyp, anyp],
        out_specs=(anyp, anyp, anyp),
        scratch_shapes=[dma((4, heads))],
        compiler_params=pltpu.CompilerParams(vmem_limit_bytes=2**20),
        name="place",
    )(gat, *(pltpu.with_memory_space_constraint(a, pltpu.VMEM) for a in raw))


def solution(mesh):
    in_specs = (
        P(("rep", "tp"), "sub"),
        P(("rep", "sub"), "tp"),
        P(("rep", "sub"), "tp"),
        P(),
        P(),
        P(),
    )
    out_specs = (P(("rep", "sub"), "tp"), P(("rep", "sub"), "tp"), P(("rep", "sub"), "tp"))
    return jax.shard_map(
        functools.partial(per_device, mesh.shape["tp"], mesh.shape["sub"]),
        mesh=mesh, in_specs=in_specs, out_specs=out_specs, check_vma=False)
```

```python
import functools

import jax
import jax.numpy as jnp
from jax import lax
from jax.experimental import pallas as pl
from jax.experimental.pallas import tpu as pltpu
from jax.sharding import PartitionSpec as P

HD = 128
F32, BF16 = jnp.float32, jnp.bfloat16
FILL = 16
FILL1, FILL2 = 2, 3
Q1 = 2
AHEAD = 2


def distances(tp, heads):
    capacity = max(2, heads // tp)
    select = heads // capacity
    stride = tp // select
    return [min(1, stride - 1)] + [k * stride for k in range(1, select)], capacity, stride


def routes(tp, t, heads, mine_ref, other_ref, out):
    _, cap, stride = distances(tp, heads)
    wanted = [mine_ref[t * heads + i] for i in range(heads)]

    def look(p, found):
        head = other_ref[p]
        return tuple(jnp.where(head == w, p, f) for w, f in zip(wanted, found))

    at = lax.fori_loop(0, heads * tp, look, (jnp.int32(0),) * heads, unroll=8)
    hops = []
    for pos in at:
        d = lax.rem(pos // heads - t + tp, tp)
        d = d if out else lax.rem(tp - d, tp)
        hops.append(jnp.where(lax.rem(d, stride) == 0, d // stride, 0))
    first = list(range(heads)) if out else at
    ranks = []
    for i in range(heads):
        before = [jnp.where((hops[j] == hops[i]) & (first[j] < first[i]), 1, 0) for j in range(heads) if j != i]
        ranks.append(hops[i] * cap + sum(before))
    return ranks


def mul(index, size):
    return pl.multiple_of(index * size, size)


def exchange(tp, subs, src_ref, tgt_ref, kvt_ref, acts_ref, q_ref, kv_ref, qraw, kvraw, sraw, kvres, gat_ref,
             gat, acts, qv, sendq, kvown, kvbuf, kvsend, part, rsbuf, res, ld, asend, arecv, apsend, aprecv,
             k1send, k1recv, k2send, k2recv, qsend, qrecv, rsend, rrecv, ss_send, ss_recv):
    t, x = lax.axis_index("tp"), lax.axis_index("sub")
    core, y = lax.rem(t, 2), t // 2
    ring = tp // 2
    full = ring // 2 - 1
    toks, rows = acts_ref.shape[0], q_ref.shape[0]
    heads = q_ref.shape[1] // HD
    pairs = heads // 2
    dist, cap, _ = distances(tp, heads)
    far = len(dist) // 2
    near = [k for k in range(1, len(dist)) if k != far]
    mate = t + 1 - 2 * core
    piece = rows // ring
    block = acts.shape[0] // subs

    def at(d):
        return lax.rem(t + d + 2 * tp, tp)

    def chip(d):
        return lax.rem(y + d + ring, ring)

    def describe(src, dst, send, recv, **where):
        return pltpu.make_async_remote_copy(
            src_ref=src, dst_ref=dst, send_sem=send, recv_sem=recv, device_id=where)

    def remote(src, dst, send, recv, **where):
        describe(src, dst, send, recv, **where).start()

    def arrived(dst, send, recv):
        describe(dst, dst, send, recv, tp=t).wait_recv()

    def tokens_of(index):
        return acts.at[pl.ds(mul(index, toks), toks)]

    def rows_of(index):
        return pl.ds(mul(index, piece), piece)

    loads = [
        pltpu.make_async_copy(acts_ref, tokens_of(t), ld.at[0]),
        pltpu.make_async_copy(kv_ref, kvown, ld.at[1]),
        pltpu.make_async_copy(kv_ref.at[rows_of(y)], kvbuf.at[y], ld.at[2]),
    ] + [pltpu.make_async_copy(q_ref.at[:, pl.ds(i * HD, HD)], qv.at[i], ld.at[3]) for i in range(heads)]
    for copy in loads:
        copy.start()
    barrier = pltpu.get_barrier_semaphore()
    for peer in (at(2), at(-2), mate):
        pl.semaphore_signal(barrier, inc=1, device_id={"tp": peer})
    for d in (1, subs - 1):
        pl.semaphore_signal(barrier, inc=1, device_id={"sub": lax.rem(x + d, subs)})
    for copy in loads[:3]:
        copy.wait()
    with jax.named_scope("barrier"):
        pl.semaphore_wait(barrier, 5)

    def tokens(d, step, origin):
        remote(tokens_of(origin), tokens_of(origin), asend, arecv.at[d, step], tp=at(2 - 4 * d))

    def hand(k, origin):
        remote(tokens_of(origin), tokens_of(origin), apsend, aprecv.at[k], tp=mate)

    def handed(k, origin):
        arrived(tokens_of(origin + 1 - 2 * core), apsend, aprecv.at[k])

    tokens(0, 0, t)
    tokens(1, 0, t)
    hand(0, t)
    def first_leg(d):
        remote(kvown.at[rows_of(chip(d))], kvbuf.at[y], k1send, k1recv, tp=at(2 * d))

    first_leg(1)
    first_leg(-1)

    place_of = routes(tp, t, heads, src_ref, tgt_ref, True)
    picks = [sum(jnp.where(r == i, slot, 0) for slot, r in enumerate(place_of)) for i in range(heads)]
    pltpu.make_async_copy(qv, qv, ld.at[3]).wait()
    with jax.named_scope("select"):
        for i in range(heads):
            sendq[i] = qv[picks[i]]

    fills = []
    per_head = FILL // cap
    span = rows // per_head

    def fill(count):
        start = len(fills)
        for n in range(start, min(start + count, FILL)):
            fills.append(n)
            for f, k in enumerate(near):
                head, cut = k * cap + n // per_head, pl.ds(n % per_head * span, span)
                remote(sendq.at[head, cut], qraw.at[head, cut], qsend, qrecv, tp=at(dist[k]))

    def straight(k):
        for i in range(k * cap, (k + 1) * cap):
            remote(sendq.at[i], qraw.at[i], qsend, qrecv, tp=at(dist[k]))

    def second_leg():
        with jax.named_scope("leg1"):
            arrived(kvbuf.at[pl.ds(1, ring - 1)], k1send, k1recv)
        for d in range(1, tp):
            kvsend[d] = kvbuf[kvt_ref[at(d)]]
        kvraw[core, rows_of(y), :] = kvbuf[kvt_ref[t]]
        for d in sorted(range(1, tp), key=lambda d: -min(d, tp - d)):
            remote(kvsend.at[d], kvraw.at[core, rows_of(y)], k2send, k2recv, tp=at(d))

    for step in range(1, full + 2):
        for d in (0, 1):
            if step > full + d:
                continue
            origin = at(-2 * step) if d == 0 else at(2 * step)
            with jax.named_scope(f"tokens{step}{d}"):
                arrived(tokens_of(origin), asend, arecv.at[d, step - 1])
            if step < full + d:
                tokens(d, step, origin)
            hand(2 * step - 1 + d if step <= full else ring - 1, origin)
            if step > 1:
                first_leg(-step if d == 0 else step)
        if step > 1:
            fill(FILL1)
        if step == Q1:
            with jax.named_scope("next"):
                handed(0, t)
                handed(2, at(2))
            straight(0)

    tile = 256

    def product(j, ref, first):
        with jax.named_scope(f"product{j}"):
            @pl.loop(0, acts.shape[0] // tile)
            def _(m):
                r = pl.ds(mul(m, tile), tile)
                rhs = jnp.concatenate([ref[first], ref[first + 1]], axis=1)
                p = jnp.dot(acts[r, :], rhs, preferred_element_type=F32)
                part[j, 0, r, :] = p[:, :HD]
                part[j, 1, r, :] = p[:, HD:]
        for d in (0, 1):
            rs_copy(j, d, 0).start()

    def part_of(b):
        return pl.ds(mul(b, block), block)

    def rs_copy(j, d, s):
        b = lax.rem(x - 1 - s + 2 * subs, subs) if d == 0 else lax.rem(x + 1 + s, subs)
        return describe(part.at[j, d, part_of(b)], rsbuf.at[j, d, s], rsend.at[j, d], rrecv.at[j, d, s],
                        sub=lax.rem(x + (1 if d == 0 else subs - 1), subs))

    def rs_step(group):
        with jax.named_scope(f"reduce{group[-1][1]}"):
            ready = None
            for j, s in group:
                for d in (0, 1):
                    b = lax.rem(x - 2 - s + 2 * subs, subs) if d == 0 else lax.rem(x + 2 + s, subs)
                    rs_copy(j, d, s).wait_recv()
                    total = part[j, d, part_of(b), :] + rsbuf[j, d, s]
                    if s == subs - 2:
                        total = total.astype(BF16)
                        if j == pairs:
                            kvres[d] = total
                        else:
                            res[2 * j + d] = total
                        continue
                    part[j, d, part_of(b), :] = total
                    rs_copy(j, d, s).wait_send()
                    if ready is not None:
                        rs_copy(*ready).start()
                    ready = j, d, s + 1
            if ready is not None:
                rs_copy(*ready).start()

    with jax.named_scope("mate"):
        for step in range(1, full + 1):
            handed(2 * step - 1, at(-2 * step))
            if step > 1:
                handed(2 * step, at(2 * step))
        handed(ring - 1, at(ring))
    second_leg()
    fill(FILL2)

    for k in range(pairs):
        product(k, sendq, k * cap)
    for s in range(AHEAD):
        rs_step([(k, s) for k in range(pairs)])
    with jax.named_scope("leg2"):
        arrived(kvsend.at[pl.ds(1, tp - 1)], k2send, k2recv)
    fill(FILL)
    straight(far)
    product(pairs, kvraw, 0)
    for s in range(subs - 1):
        rs_step([(k, s + AHEAD) for k in range(pairs) if s + AHEAD < subs - 1] + [(pairs, s)])
        if s + AHEAD == subs - 2:
            for i in range(heads):
                remote(res.at[i], sraw.at[i], ss_send, ss_recv, tp=at(dist[i // cap]))
    for i, r in enumerate(routes(tp, t, heads, tgt_ref, src_ref, False)):
        gat[i] = r
    table = pltpu.make_async_copy(gat, gat_ref, ld.at[0])
    table.start()
    for j in range(pairs + 1):
        for d in (0, 1):
            rs_copy(j, d, subs - 2).wait_send()

    table.wait()
    with jax.named_scope("sent"):
        for src, sem in ((acts.at[pl.ds(0, (2 * full + 1) * toks)], asend), (acts.at[pl.ds(0, ring * toks)], apsend),
                         (kvbuf.at[pl.ds(1, ring - 1)], k1send), (kvsend.at[pl.ds(1, tp - 1)], k2send),
                         (sendq, qsend), (res, ss_send)):
            describe(src, src, sem, sem, tp=t).wait_send()
    with jax.named_scope("heads"):
        arrived(qraw, qsend, qrecv)
    with jax.named_scope("back"):
        arrived(sraw, ss_send, ss_recv)


def place(gat, qraw, kvraw, sraw, kvres, q_new, kv_new, qkv, sem):
    heads = qraw.shape[0]
    copies = []
    for p in range(heads):
        cols = pl.ds(p * HD, HD)
        copies.append(pltpu.make_async_copy(qraw.at[gat[p]], q_new.at[:, cols], sem.at[0, p]))
        copies.append(pltpu.make_async_copy(sraw.at[gat[p]], qkv.at[:, cols], sem.at[1, p]))
    for p in range(2):
        copies.append(pltpu.make_async_copy(kvraw.at[p], kv_new.at[:, pl.ds(p * HD, HD)], sem.at[2, p]))
        copies.append(pltpu.make_async_copy(kvres.at[p], qkv.at[:, pl.ds((heads + p) * HD, HD)], sem.at[3, p]))
    for copy in copies:
        copy.start()
    for copy in copies:
        copy.wait()


def per_device(tp, subs, acts, q_src, kv_src, q_src_heads, q_tgt_heads, kv_tgt_heads):
    toks, depth = acts.shape
    rows, heads = q_src.shape[0], q_src.shape[1] // HD
    dist, _, _ = distances(tp, heads)
    wide = rows, HD
    tokens = toks * tp
    block = tokens // subs
    ring = tp // 2
    full = ring // 2 - 1
    dma = pltpu.SemaphoreType.DMA
    vmem = pl.BlockSpec(memory_space=pltpu.VMEM)
    smem = pl.BlockSpec(memory_space=pltpu.SMEM)
    anyp = pl.BlockSpec(memory_space=pl.ANY)
    *raw, gat = pl.pallas_call(
        functools.partial(exchange, tp, subs),
        out_shape=(
            pltpu.VMEM((heads, *wide), BF16),
            pltpu.VMEM((2, *wide), BF16),
            pltpu.VMEM((heads, block, HD), BF16),
            pltpu.VMEM((2, block, HD), BF16),
            jax.ShapeDtypeStruct((heads,), jnp.int32),
        ),
        in_specs=[smem, smem, smem, anyp, anyp, anyp],
        out_specs=(vmem, vmem, vmem, vmem, anyp),
        scratch_shapes=[
            pltpu.SMEM((heads,), jnp.int32),
            pltpu.VMEM((tokens, depth), BF16),
            pltpu.VMEM((heads, *wide), BF16),
            pltpu.VMEM((heads, *wide), BF16),
            pltpu.VMEM(wide, BF16),
            pltpu.VMEM((ring, rows // ring, HD), BF16),
            pltpu.VMEM((tp, rows // ring, HD), BF16),
            pltpu.VMEM((heads // 2 + 1, 2, tokens, HD), F32),
            pltpu.VMEM((heads // 2 + 1, 2, subs - 1, block, HD), F32),
            pltpu.VMEM((heads, block, HD), BF16),
            dma((4,)),
            dma,
            dma((2, full + 1)),
            dma,
            dma((ring,)),
            *[dma] * 6,
            dma((heads // 2 + 1, 2)),
            dma((heads // 2 + 1, 2, subs - 1)),
            dma,
            dma,
        ],
        compiler_params=pltpu.CompilerParams(
            collective_id=0, has_side_effects=True, vmem_limit_bytes=50 * 2**20),
        name="exchange",
    )(q_src_heads, q_tgt_heads, kv_tgt_heads, acts, q_src, kv_src)
    return pl.pallas_call(
        place,
        out_shape=(
            jax.ShapeDtypeStruct(q_src.shape, BF16),
            jax.ShapeDtypeStruct((rows, 2 * HD), BF16),
            jax.ShapeDtypeStruct((block, (heads + 2) * HD), BF16),
        ),
        in_specs=[smem, anyp, anyp, anyp, anyp],
        out_specs=(anyp, anyp, anyp),
        scratch_shapes=[dma((4, heads))],
        compiler_params=pltpu.CompilerParams(vmem_limit_bytes=2**20),
        name="place",
    )(gat, *(pltpu.with_memory_space_constraint(a, pltpu.VMEM) for a in raw))


def solution(mesh):
    in_specs = (
        P(("rep", "tp"), "sub"),
        P(("rep", "sub"), "tp"),
        P(("rep", "sub"), "tp"),
        P(),
        P(),
        P(),
    )
    out_specs = (P(("rep", "sub"), "tp"), P(("rep", "sub"), "tp"), P(("rep", "sub"), "tp"))
    return jax.shard_map(
        functools.partial(per_device, mesh.shape["tp"], mesh.shape["sub"]),
        mesh=mesh, in_specs=in_specs, out_specs=out_specs, check_vma=False)
```

```python
import functools

import jax
import jax.numpy as jnp
from jax import lax
from jax.experimental import pallas as pl
from jax.experimental.pallas import tpu as pltpu
from jax.sharding import PartitionSpec as P

HD = 128
F32, BF16 = jnp.float32, jnp.bfloat16
FILL = 16
FILL1, FILL2 = 2, 3
Q1 = 2
AHEAD = 2


def distances(tp, heads):
    capacity = max(2, heads // tp)
    select = heads // capacity
    stride = tp // select
    return [min(1, stride - 1)] + [k * stride for k in range(1, select)], capacity, stride


def routes(tp, t, heads, mine_ref, other_ref, out):
    _, cap, stride = distances(tp, heads)
    wanted = [mine_ref[t * heads + i] for i in range(heads)]

    def look(p, found):
        head = other_ref[p]
        return tuple(jnp.where(head == w, p, f) for w, f in zip(wanted, found))

    at = lax.fori_loop(0, heads * tp, look, (jnp.int32(0),) * heads, unroll=8)
    hops = []
    for pos in at:
        d = lax.rem(pos // heads - t + tp, tp)
        d = d if out else lax.rem(tp - d, tp)
        hops.append(jnp.where(lax.rem(d, stride) == 0, d // stride, 0))
    first = list(range(heads)) if out else at
    ranks = []
    for i in range(heads):
        before = [jnp.where((hops[j] == hops[i]) & (first[j] < first[i]), 1, 0) for j in range(heads) if j != i]
        ranks.append(hops[i] * cap + sum(before))
    return ranks


def mul(index, size):
    return pl.multiple_of(index * size, size)


def exchange(tp, subs, src_ref, tgt_ref, kvt_ref, acts_ref, q_ref, kv_ref, qraw, kvraw, sraw, kvres, gat,
             acts, qv, sendq, kvown, kvbuf, kvsend, relay, part, rsbuf, res, ld, asend, arecv, apsend, aprecv,
             k1send, k1recv, k2send, k2recv, qsend, qrecv, rsend, rrecv, ss_send, ss_recv, hsend, hrecv):
    t, x = lax.axis_index("tp"), lax.axis_index("sub")
    core, y = lax.rem(t, 2), t // 2
    ring = tp // 2
    full = ring // 2 - 1
    toks, rows = acts_ref.shape[0], q_ref.shape[0]
    heads = q_ref.shape[1] // HD
    pairs = heads // 2
    dist, cap, _ = distances(tp, heads)
    far = len(dist) // 2
    near = [k for k in range(1, len(dist)) if k != far]
    mate = t + 1 - 2 * core
    piece = rows // ring
    block = acts.shape[0] // subs

    def at(d):
        return lax.rem(t + d + 2 * tp, tp)

    def chip(d):
        return lax.rem(y + d + ring, ring)

    def describe(src, dst, send, recv, **where):
        return pltpu.make_async_remote_copy(
            src_ref=src, dst_ref=dst, send_sem=send, recv_sem=recv, device_id=where)

    def remote(src, dst, send, recv, **where):
        describe(src, dst, send, recv, **where).start()

    def arrived(dst, send, recv):
        describe(dst, dst, send, recv, tp=t).wait_recv()

    def tokens_of(index):
        return acts.at[pl.ds(mul(index, toks), toks)]

    def rows_of(index):
        return pl.ds(mul(index, piece), piece)

    loads = [
        pltpu.make_async_copy(acts_ref, tokens_of(t), ld.at[0]),
        pltpu.make_async_copy(kv_ref, kvown, ld.at[1]),
        pltpu.make_async_copy(kv_ref.at[rows_of(y)], kvbuf.at[y], ld.at[2]),
    ] + [pltpu.make_async_copy(q_ref.at[:, pl.ds(i * HD, HD)], qv.at[i], ld.at[3]) for i in range(heads)]
    for copy in loads:
        copy.start()
    barrier = pltpu.get_barrier_semaphore()
    for peer in (at(2), at(-2), mate):
        pl.semaphore_signal(barrier, inc=1, device_id={"tp": peer})
    for d in (1, subs - 1):
        pl.semaphore_signal(barrier, inc=1, device_id={"sub": lax.rem(x + d, subs)})
    for copy in loads[:3]:
        copy.wait()
    with jax.named_scope("barrier"):
        pl.semaphore_wait(barrier, 5)

    def tokens(d, step, origin):
        remote(tokens_of(origin), tokens_of(origin), asend, arecv.at[d, step], tp=at(2 - 4 * d))

    def hand(k, origin):
        remote(tokens_of(origin), tokens_of(origin), apsend, aprecv.at[k], tp=mate)

    def handed(k, origin):
        arrived(tokens_of(origin + 1 - 2 * core), apsend, aprecv.at[k])

    tokens(0, 0, t)
    tokens(1, 0, t)
    hand(0, t)
    def first_leg(d):
        remote(kvown.at[rows_of(chip(d))], kvbuf.at[y], k1send, k1recv, tp=at(2 * d))

    first_leg(1)
    first_leg(-1)

    place_of = routes(tp, t, heads, src_ref, tgt_ref, True)
    picks = [sum(jnp.where(r == i, slot, 0) for slot, r in enumerate(place_of)) for i in range(heads)]
    pltpu.make_async_copy(qv, qv, ld.at[3]).wait()
    with jax.named_scope("select"):
        for i in range(heads):
            sendq[i] = qv[picks[i]]

    fills = []
    per_head = FILL // cap
    span = rows // per_head

    def fill(count):
        start = len(fills)
        for n in range(start, min(start + count, FILL)):
            fills.append(n)
            for f, k in enumerate(near):
                head, cut = k * cap + n // per_head, pl.ds(n % per_head * span, span)
                remote(sendq.at[head, cut], qraw.at[head, cut], qsend, qrecv, tp=at(dist[k]))

    def straight(k):
        for i in range(k * cap, (k + 1) * cap):
            whole = pl.ds(0, rows - (piece if k == far and i == detour else 0))
            remote(sendq.at[i, whole], qraw.at[i, whole], qsend, qrecv, tp=at(dist[k]))

    detour, end = (far + 1) * cap - 1, pl.ds(rows - piece, piece)

    def second_leg():
        with jax.named_scope("leg1"):
            arrived(kvbuf.at[pl.ds(1, ring - 1)], k1send, k1recv)
        for d in range(1, tp):
            kvsend[d] = kvbuf[kvt_ref[at(d)]]
        kvraw[core, rows_of(y), :] = kvbuf[kvt_ref[t]]
        for d in sorted(range(1, tp), key=lambda d: -min(d, tp - d)):
            remote(kvsend.at[d], kvraw.at[core, rows_of(y)], k2send, k2recv, tp=at(d))

    for step in range(1, full + 2):
        for d in (0, 1):
            if step > full + d:
                continue
            origin = at(-2 * step) if d == 0 else at(2 * step)
            with jax.named_scope(f"tokens{step}{d}"):
                arrived(tokens_of(origin), asend, arecv.at[d, step - 1])
            if step < full + d:
                tokens(d, step, origin)
            hand(2 * step - 1 + d if step <= full else ring - 1, origin)
            if step > 1:
                first_leg(-step if d == 0 else step)
        if step > 1:
            fill(FILL1)
        if step == Q1:
            with jax.named_scope("next"):
                handed(0, t)
                handed(2, at(2))
            straight(0)

    tile = 256

    def product(j, ref, first):
        with jax.named_scope(f"product{j}"):
            @pl.loop(0, acts.shape[0] // tile)
            def _(m):
                r = pl.ds(mul(m, tile), tile)
                rhs = jnp.concatenate([ref[first], ref[first + 1]], axis=1)
                p = jnp.dot(acts[r, :], rhs, preferred_element_type=F32)
                part[j, 0, r, :] = p[:, :HD]
                part[j, 1, r, :] = p[:, HD:]
        for d in (0, 1):
            rs_copy(j, d, 0).start()

    def part_of(b):
        return pl.ds(mul(b, block), block)

    def rs_copy(j, d, s):
        b = lax.rem(x - 1 - s + 2 * subs, subs) if d == 0 else lax.rem(x + 1 + s, subs)
        return describe(part.at[j, d, part_of(b)], rsbuf.at[j, d, s], rsend.at[j, d], rrecv.at[j, d, s],
                        sub=lax.rem(x + (1 if d == 0 else subs - 1), subs))

    def rs_step(group):
        with jax.named_scope(f"reduce{group[-1][1]}"):
            ready = None
            for j, s in group:
                for d in (0, 1):
                    b = lax.rem(x - 2 - s + 2 * subs, subs) if d == 0 else lax.rem(x + 2 + s, subs)
                    rs_copy(j, d, s).wait_recv()
                    total = part[j, d, part_of(b), :] + rsbuf[j, d, s]
                    if s == subs - 2:
                        total = total.astype(BF16)
                        if j == pairs:
                            kvres[d] = total
                        else:
                            res[2 * j + d] = total
                        continue
                    part[j, d, part_of(b), :] = total
                    rs_copy(j, d, s).wait_send()
                    if ready is not None:
                        rs_copy(*ready).start()
                    ready = j, d, s + 1
            if ready is not None:
                rs_copy(*ready).start()

    with jax.named_scope("mate"):
        for step in range(1, full + 1):
            handed(2 * step - 1, at(-2 * step))
            if step > 1:
                handed(2 * step, at(2 * step))
        handed(ring - 1, at(ring))
    remote(sendq.at[detour, end], relay, qsend, hrecv, tp=at(-2))
    second_leg()
    fill(FILL2)

    for k in range(pairs):
        product(k, sendq, k * cap)
    for s in range(AHEAD):
        rs_step([(k, s) for k in range(pairs)])
    with jax.named_scope("leg2"):
        arrived(kvsend.at[pl.ds(1, tp - 1)], k2send, k2recv)
    arrived(relay, hsend, hrecv)
    remote(relay, qraw.at[detour, end], hsend, qrecv, tp=at(2 - dist[far]))
    fill(FILL)
    straight(far)
    product(pairs, kvraw, 0)
    for s in range(subs - 1):
        rs_step([(k, s + AHEAD) for k in range(pairs) if s + AHEAD < subs - 1] + [(pairs, s)])
        if s + AHEAD == subs - 2:
            for i in range(heads):
                remote(res.at[i], sraw.at[i], ss_send, ss_recv, tp=at(dist[i // cap]))
    for i, r in enumerate(routes(tp, t, heads, tgt_ref, src_ref, False)):
        gat[i] = r
    for j in range(pairs + 1):
        for d in (0, 1):
            rs_copy(j, d, subs - 2).wait_send()

    with jax.named_scope("sent"):
        for src, sem in ((acts.at[pl.ds(0, (2 * full + 1) * toks)], asend), (acts.at[pl.ds(0, ring * toks)], apsend),
                         (kvbuf.at[pl.ds(1, ring - 1)], k1send), (kvsend.at[pl.ds(1, tp - 1)], k2send),
                         (sendq, qsend), (res, ss_send), (relay, hsend)):
            describe(src, src, sem, sem, tp=t).wait_send()
    with jax.named_scope("heads"):
        arrived(qraw, qsend, qrecv)
    with jax.named_scope("back"):
        arrived(sraw, ss_send, ss_recv)


def place(gat, qraw, kvraw, sraw, kvres, q_new, kv_new, qkv, sem):
    heads = qraw.shape[0]
    copies = []
    for p in range(heads):
        cols = pl.ds(p * HD, HD)
        copies.append(pltpu.make_async_copy(qraw.at[gat[p]], q_new.at[:, cols], sem.at[0, p]))
        copies.append(pltpu.make_async_copy(sraw.at[gat[p]], qkv.at[:, cols], sem.at[1, p]))
    for p in range(2):
        copies.append(pltpu.make_async_copy(kvraw.at[p], kv_new.at[:, pl.ds(p * HD, HD)], sem.at[2, p]))
        copies.append(pltpu.make_async_copy(kvres.at[p], qkv.at[:, pl.ds((heads + p) * HD, HD)], sem.at[3, p]))
    for copy in copies:
        copy.start()
    for copy in copies:
        copy.wait()


def per_device(tp, subs, acts, q_src, kv_src, q_src_heads, q_tgt_heads, kv_tgt_heads):
    toks, depth = acts.shape
    rows, heads = q_src.shape[0], q_src.shape[1] // HD
    dist, _, _ = distances(tp, heads)
    wide = rows, HD
    tokens = toks * tp
    block = tokens // subs
    ring = tp // 2
    full = ring // 2 - 1
    dma = pltpu.SemaphoreType.DMA
    vmem = pl.BlockSpec(memory_space=pltpu.VMEM)
    smem = pl.BlockSpec(memory_space=pltpu.SMEM)
    anyp = pl.BlockSpec(memory_space=pl.ANY)
    *raw, gat = pl.pallas_call(
        functools.partial(exchange, tp, subs),
        out_shape=(
            pltpu.VMEM((heads, *wide), BF16),
            pltpu.VMEM((2, *wide), BF16),
            pltpu.VMEM((heads, block, HD), BF16),
            pltpu.VMEM((2, block, HD), BF16),
            pltpu.SMEM((heads,), jnp.int32),
        ),
        in_specs=[smem, smem, smem, anyp, anyp, anyp],
        out_specs=(vmem, vmem, vmem, vmem, smem),
        scratch_shapes=[
            pltpu.VMEM((tokens, depth), BF16),
            pltpu.VMEM((heads, *wide), BF16),
            pltpu.VMEM((heads, *wide), BF16),
            pltpu.VMEM(wide, BF16),
            pltpu.VMEM((ring, rows // ring, HD), BF16),
            pltpu.VMEM((tp, rows // ring, HD), BF16),
            pltpu.VMEM((rows // ring, HD), BF16),
            pltpu.VMEM((heads // 2 + 1, 2, tokens, HD), F32),
            pltpu.VMEM((heads // 2 + 1, 2, subs - 1, block, HD), F32),
            pltpu.VMEM((heads, block, HD), BF16),
            dma((4,)),
            dma,
            dma((2, full + 1)),
            dma,
            dma((ring,)),
            *[dma] * 6,
            dma((heads // 2 + 1, 2)),
            dma((heads // 2 + 1, 2, subs - 1)),
            dma,
            dma,
            dma,
            dma,
        ],
        compiler_params=pltpu.CompilerParams(
            collective_id=0, has_side_effects=True, vmem_limit_bytes=50 * 2**20),
        name="exchange",
    )(q_src_heads, q_tgt_heads, kv_tgt_heads, acts, q_src, kv_src)
    return pl.pallas_call(
        place,
        out_shape=(
            jax.ShapeDtypeStruct(q_src.shape, BF16),
            jax.ShapeDtypeStruct((rows, 2 * HD), BF16),
            jax.ShapeDtypeStruct((block, (heads + 2) * HD), BF16),
        ),
        in_specs=[smem, anyp, anyp, anyp, anyp],
        out_specs=(anyp, anyp, anyp),
        scratch_shapes=[dma((4, heads))],
        compiler_params=pltpu.CompilerParams(vmem_limit_bytes=2**20),
        name="place",
    )(pltpu.with_memory_space_constraint(gat, pltpu.SMEM), *(pltpu.with_memory_space_constraint(a, pltpu.VMEM) for a in raw))


def solution(mesh):
    in_specs = (
        P(("rep", "tp"), "sub"),
        P(("rep", "sub"), "tp"),
        P(("rep", "sub"), "tp"),
        P(),
        P(),
        P(),
    )
    out_specs = (P(("rep", "sub"), "tp"), P(("rep", "sub"), "tp"), P(("rep", "sub"), "tp"))
    return jax.shard_map(
        functools.partial(per_device, mesh.shape["tp"], mesh.shape["sub"]),
        mesh=mesh, in_specs=in_specs, out_specs=out_specs, check_vma=False)
```

```python
import functools

import jax
import jax.numpy as jnp
from jax import lax
from jax.experimental import pallas as pl
from jax.experimental.pallas import tpu as pltpu
from jax.sharding import PartitionSpec as P

HD = 128
F32, BF16 = jnp.float32, jnp.bfloat16
FILL = 16
FILL1, FILL2 = 2, 3
Q1 = 2
AHEAD = 2


def distances(tp, heads):
    capacity = max(2, heads // tp)
    select = heads // capacity
    stride = tp // select
    return [min(1, stride - 1)] + [k * stride for k in range(1, select)], capacity, stride


def routes(tp, t, heads, mine_ref, other_ref, out):
    _, cap, stride = distances(tp, heads)
    wanted = [mine_ref[t * heads + i] for i in range(heads)]

    def look(p, found):
        head = other_ref[p]
        return tuple(jnp.where(head == w, p, f) for w, f in zip(wanted, found))

    at = lax.fori_loop(0, heads * tp, look, (jnp.int32(0),) * heads, unroll=8)
    hops = []
    for pos in at:
        d = lax.rem(pos // heads - t + tp, tp)
        d = d if out else lax.rem(tp - d, tp)
        hops.append(jnp.where(lax.rem(d, stride) == 0, d // stride, 0))
    first = list(range(heads)) if out else at
    ranks = []
    for i in range(heads):
        before = [jnp.where((hops[j] == hops[i]) & (first[j] < first[i]), 1, 0) for j in range(heads) if j != i]
        ranks.append(hops[i] * cap + sum(before))
    return ranks


def mul(index, size):
    return pl.multiple_of(index * size, size)


def exchange(tp, subs, src_ref, tgt_ref, kvt_ref, acts_ref, q_ref, kv_ref, qraw, kvraw, sraw, kvres, gat,
             acts, qv, sendq, kvown, kvbuf, kvsend, relay, part, rsbuf, res, ld, asend, arecv, apsend, aprecv,
             k1send, k1recv, k2send, k2recv, qsend, qrecv, rsend, rrecv, ss_send, ss_recv, hsend, hrecv):
    t, x = lax.axis_index("tp"), lax.axis_index("sub")
    core, y = lax.rem(t, 2), t // 2
    ring = tp // 2
    full = ring // 2 - 1
    toks, rows = acts_ref.shape[0], q_ref.shape[0]
    heads = q_ref.shape[1] // HD
    pairs = heads // 2
    dist, cap, _ = distances(tp, heads)
    far = len(dist) // 2
    near = [k for k in range(1, len(dist)) if k != far]
    mate = t + 1 - 2 * core
    piece = rows // ring
    block = acts.shape[0] // subs

    def at(d):
        return lax.rem(t + d + 2 * tp, tp)

    def chip(d):
        return lax.rem(y + d + ring, ring)

    def describe(src, dst, send, recv, **where):
        return pltpu.make_async_remote_copy(
            src_ref=src, dst_ref=dst, send_sem=send, recv_sem=recv, device_id=where)

    def remote(src, dst, send, recv, **where):
        describe(src, dst, send, recv, **where).start()

    def arrived(dst, send, recv):
        describe(dst, dst, send, recv, tp=t).wait_recv()

    def tokens_of(index):
        return acts.at[pl.ds(mul(index, toks), toks)]

    def rows_of(index):
        return pl.ds(mul(index, piece), piece)

    loads = [
        pltpu.make_async_copy(acts_ref, tokens_of(t), ld.at[0]),
        pltpu.make_async_copy(kv_ref, kvown, ld.at[1]),
        pltpu.make_async_copy(kv_ref.at[rows_of(y)], kvbuf.at[y], ld.at[2]),
    ] + [pltpu.make_async_copy(q_ref.at[:, pl.ds(i * HD, HD)], qv.at[i], ld.at[3]) for i in range(heads)]
    for copy in loads:
        copy.start()
    barrier = pltpu.get_barrier_semaphore()
    for peer in (at(2), at(-2)):
        pl.semaphore_signal(barrier, inc=1, device_id={"tp": peer})

    @pl.when(core == 1)
    def _():
        pl.semaphore_signal(barrier, inc=1, device_id={"tp": mate})

    for d in (1, subs - 1):
        pl.semaphore_signal(barrier, inc=1, device_id={"sub": lax.rem(x + d, subs)})
    for copy in loads[:3]:
        copy.wait()
    with jax.named_scope("barrier"):
        pl.semaphore_wait(barrier, 5 - core)

    def tokens(d, step, origin):
        remote(tokens_of(origin), tokens_of(origin), asend, arecv.at[d, step], tp=at(2 - 4 * d))

    def hand(k, origin):
        remote(tokens_of(origin), tokens_of(origin), apsend, aprecv.at[k], tp=mate)

    def handed(k, origin):
        arrived(tokens_of(origin + 1 - 2 * core), apsend, aprecv.at[k])

    tokens(0, 0, t)
    tokens(1, 0, t)
    @pl.when(core == 0)
    def _():
        hand(0, t)

    waiting = []
    def first_leg(d):
        remote(kvown.at[rows_of(chip(d))], kvbuf.at[y], k1send, k1recv, tp=at(2 * d))

    first_leg(1)
    first_leg(-1)

    place_of = routes(tp, t, heads, src_ref, tgt_ref, True)
    picks = [sum(jnp.where(r == i, slot, 0) for slot, r in enumerate(place_of)) for i in range(heads)]
    pltpu.make_async_copy(qv, qv, ld.at[3]).wait()
    with jax.named_scope("select"):
        for i in range(heads):
            sendq[i] = qv[picks[i]]

    fills = []
    per_head = FILL // cap
    span = rows // per_head

    def fill(count):
        start = len(fills)
        for n in range(start, min(start + count, FILL)):
            fills.append(n)
            for f, k in enumerate(near):
                head, cut = k * cap + n // per_head, pl.ds(n % per_head * span, span)
                remote(sendq.at[head, cut], qraw.at[head, cut], qsend, qrecv, tp=at(dist[k]))

    def straight(k):
        for i in range(k * cap, (k + 1) * cap):
            whole = pl.ds(0, rows - (piece if k == far and i == detour else 0))
            remote(sendq.at[i, whole], qraw.at[i, whole], qsend, qrecv, tp=at(dist[k]))

    detour, end = (far + 1) * cap - 1, pl.ds(rows - piece, piece)

    def second_leg():
        with jax.named_scope("leg1"):
            arrived(kvbuf.at[pl.ds(1, ring - 1)], k1send, k1recv)
        for d in range(1, tp):
            kvsend[d] = kvbuf[kvt_ref[at(d)]]
        kvraw[core, rows_of(y), :] = kvbuf[kvt_ref[t]]
        for d in sorted(range(1, tp), key=lambda d: -min(d, tp - d)):
            remote(kvsend.at[d], kvraw.at[core, rows_of(y)], k2send, k2recv, tp=at(d))

    for step in range(1, full + 2):
        for d in (0, 1):
            if step > full + d:
                continue
            origin = at(-2 * step) if d == 0 else at(2 * step)
            with jax.named_scope(f"tokens{step}{d}"):
                arrived(tokens_of(origin), asend, arecv.at[d, step - 1])
            if step < full + d:
                tokens(d, step, origin)
            turn = 2 * step - 1 + d if step <= full else ring - 1, origin
            if step <= Q1:
                waiting.append(turn)
            else:
                hand(*turn)
            if step > 1:
                first_leg(-step if d == 0 else step)
        if step > 1:
            fill(FILL1)
        if step == Q1:
            with jax.named_scope("next"):
                @pl.when(core == 1)
                def _():
                    handed(0, t)
                    hand(0, t)

                for turn in waiting:
                    hand(*turn)

                @pl.when(core == 0)
                def _():
                    handed(0, t)

                handed(2, at(2))
            straight(0)

    tile = 256

    def product(j, ref, first):
        with jax.named_scope(f"product{j}"):
            @pl.loop(0, acts.shape[0] // tile)
            def _(m):
                r = pl.ds(mul(m, tile), tile)
                rhs = jnp.concatenate([ref[first], ref[first + 1]], axis=1)
                p = jnp.dot(acts[r, :], rhs, preferred_element_type=F32)
                part[j, 0, r, :] = p[:, :HD]
                part[j, 1, r, :] = p[:, HD:]
        for d in (0, 1):
            rs_copy(j, d, 0).start()

    def part_of(b):
        return pl.ds(mul(b, block), block)

    def rs_copy(j, d, s):
        b = lax.rem(x - 1 - s + 2 * subs, subs) if d == 0 else lax.rem(x + 1 + s, subs)
        return describe(part.at[j, d, part_of(b)], rsbuf.at[j, d, s], rsend.at[j, d], rrecv.at[j, d, s],
                        sub=lax.rem(x + (1 if d == 0 else subs - 1), subs))

    def rs_step(group):
        with jax.named_scope(f"reduce{group[-1][1]}"):
            ready = None
            for j, s in group:
                for d in (0, 1):
                    b = lax.rem(x - 2 - s + 2 * subs, subs) if d == 0 else lax.rem(x + 2 + s, subs)
                    rs_copy(j, d, s).wait_recv()
                    total = part[j, d, part_of(b), :] + rsbuf[j, d, s]
                    if s == subs - 2:
                        total = total.astype(BF16)
                        if j == pairs:
                            kvres[d] = total
                        else:
                            res[2 * j + d] = total
                        continue
                    part[j, d, part_of(b), :] = total
                    rs_copy(j, d, s).wait_send()
                    if ready is not None:
                        rs_copy(*ready).start()
                    ready = j, d, s + 1
            if ready is not None:
                rs_copy(*ready).start()

    with jax.named_scope("mate"):
        for step in range(1, full + 1):
            handed(2 * step - 1, at(-2 * step))
            if step > 1:
                handed(2 * step, at(2 * step))
        handed(ring - 1, at(ring))
    remote(sendq.at[detour, end], relay, qsend, hrecv, tp=at(-2))
    second_leg()
    fill(FILL2)

    for k in range(pairs):
        product(k, sendq, k * cap)
    for s in range(AHEAD):
        rs_step([(k, s) for k in range(pairs)])
    with jax.named_scope("leg2"):
        arrived(kvsend.at[pl.ds(1, tp - 1)], k2send, k2recv)
    arrived(relay, hsend, hrecv)
    remote(relay, qraw.at[detour, end], hsend, qrecv, tp=at(2 - dist[far]))
    fill(FILL)
    straight(far)
    product(pairs, kvraw, 0)
    for s in range(subs - 1):
        rs_step([(k, s + AHEAD) for k in range(pairs) if s + AHEAD < subs - 1] + [(pairs, s)])
        if s + AHEAD == subs - 2:
            for i in range(heads):
                remote(res.at[i], sraw.at[i], ss_send, ss_recv, tp=at(dist[i // cap]))
    for i, r in enumerate(routes(tp, t, heads, tgt_ref, src_ref, False)):
        gat[i] = r
    for j in range(pairs + 1):
        for d in (0, 1):
            rs_copy(j, d, subs - 2).wait_send()

    with jax.named_scope("sent"):
        for src, sem in ((acts.at[pl.ds(0, (2 * full + 1) * toks)], asend), (acts.at[pl.ds(0, ring * toks)], apsend),
                         (kvbuf.at[pl.ds(1, ring - 1)], k1send), (kvsend.at[pl.ds(1, tp - 1)], k2send),
                         (sendq, qsend), (res, ss_send), (relay, hsend)):
            describe(src, src, sem, sem, tp=t).wait_send()
    with jax.named_scope("heads"):
        arrived(qraw, qsend, qrecv)
    with jax.named_scope("back"):
        arrived(sraw, ss_send, ss_recv)


def place(gat, qraw, kvraw, sraw, kvres, q_new, kv_new, qkv, sem):
    heads = qraw.shape[0]
    copies = []
    for p in range(heads):
        cols = pl.ds(p * HD, HD)
        copies.append(pltpu.make_async_copy(qraw.at[gat[p]], q_new.at[:, cols], sem.at[0, p]))
        copies.append(pltpu.make_async_copy(sraw.at[gat[p]], qkv.at[:, cols], sem.at[1, p]))
    for p in range(2):
        copies.append(pltpu.make_async_copy(kvraw.at[p], kv_new.at[:, pl.ds(p * HD, HD)], sem.at[2, p]))
        copies.append(pltpu.make_async_copy(kvres.at[p], qkv.at[:, pl.ds((heads + p) * HD, HD)], sem.at[3, p]))
    for copy in copies:
        copy.start()
    for copy in copies:
        copy.wait()


def per_device(tp, subs, acts, q_src, kv_src, q_src_heads, q_tgt_heads, kv_tgt_heads):
    toks, depth = acts.shape
    rows, heads = q_src.shape[0], q_src.shape[1] // HD
    dist, _, _ = distances(tp, heads)
    wide = rows, HD
    tokens = toks * tp
    block = tokens // subs
    ring = tp // 2
    full = ring // 2 - 1
    dma = pltpu.SemaphoreType.DMA
    vmem = pl.BlockSpec(memory_space=pltpu.VMEM)
    smem = pl.BlockSpec(memory_space=pltpu.SMEM)
    anyp = pl.BlockSpec(memory_space=pl.ANY)
    *raw, gat = pl.pallas_call(
        functools.partial(exchange, tp, subs),
        out_shape=(
            pltpu.VMEM((heads, *wide), BF16),
            pltpu.VMEM((2, *wide), BF16),
            pltpu.VMEM((heads, block, HD), BF16),
            pltpu.VMEM((2, block, HD), BF16),
            pltpu.SMEM((heads,), jnp.int32),
        ),
        in_specs=[smem, smem, smem, anyp, anyp, anyp],
        out_specs=(vmem, vmem, vmem, vmem, smem),
        scratch_shapes=[
            pltpu.VMEM((tokens, depth), BF16),
            pltpu.VMEM((heads, *wide), BF16),
            pltpu.VMEM((heads, *wide), BF16),
            pltpu.VMEM(wide, BF16),
            pltpu.VMEM((ring, rows // ring, HD), BF16),
            pltpu.VMEM((tp, rows // ring, HD), BF16),
            pltpu.VMEM((rows // ring, HD), BF16),
            pltpu.VMEM((heads // 2 + 1, 2, tokens, HD), F32),
            pltpu.VMEM((heads // 2 + 1, 2, subs - 1, block, HD), F32),
            pltpu.VMEM((heads, block, HD), BF16),
            dma((4,)),
            dma,
            dma((2, full + 1)),
            dma,
            dma((ring,)),
            *[dma] * 6,
            dma((heads // 2 + 1, 2)),
            dma((heads // 2 + 1, 2, subs - 1)),
            dma,
            dma,
            dma,
            dma,
        ],
        compiler_params=pltpu.CompilerParams(
            collective_id=0, has_side_effects=True, vmem_limit_bytes=50 * 2**20),
        name="exchange",
    )(q_src_heads, q_tgt_heads, kv_tgt_heads, acts, q_src, kv_src)
    return pl.pallas_call(
        place,
        out_shape=(
            jax.ShapeDtypeStruct(q_src.shape, BF16),
            jax.ShapeDtypeStruct((rows, 2 * HD), BF16),
            jax.ShapeDtypeStruct((block, (heads + 2) * HD), BF16),
        ),
        in_specs=[smem, anyp, anyp, anyp, anyp],
        out_specs=(anyp, anyp, anyp),
        scratch_shapes=[dma((4, heads))],
        compiler_params=pltpu.CompilerParams(vmem_limit_bytes=2**20),
        name="place",
    )(pltpu.with_memory_space_constraint(gat, pltpu.SMEM), *(pltpu.with_memory_space_constraint(a, pltpu.VMEM) for a in raw))


def solution(mesh):
    in_specs = (
        P(("rep", "tp"), "sub"),
        P(("rep", "sub"), "tp"),
        P(("rep", "sub"), "tp"),
        P(),
        P(),
        P(),
    )
    out_specs = (P(("rep", "sub"), "tp"), P(("rep", "sub"), "tp"), P(("rep", "sub"), "tp"))
    return jax.shard_map(
        functools.partial(per_device, mesh.shape["tp"], mesh.shape["sub"]),
        mesh=mesh, in_specs=in_specs, out_specs=out_specs, check_vma=False)
```
